32 devices in a mesh: dp: 16 (over z, y, core), rep: 2 (over x).
Axes of the slice: x: 2, y: 2, z: 4, core: 2. Of those that a mesh axis runs over, the one named last changes fastest.
Arguments:
- gate_pre: bfloat16 [2, 2048, 5632], P(None, 'dp', 'rep'), may hold values from -8 to 8
- up_pre: bfloat16 [2, 2048, 5632], P(None, 'dp', 'rep'), may hold values from -6 to 6
- out_grad: bfloat16 [2, 2048, 1024], P(None, 'dp'), may hold values from -6 to 6
- master: float32 [1024, 5632], P('dp', 'rep'), may hold values from -0.078125 to 0.078125
- moment_one: float32 [1024, 5632], P('dp', 'rep'), may hold values from -0.02 to 0.02
- moment_two: float32 [1024, 5632], P('dp', 'rep'), may hold values from 1e-06 to 1e-05
Outputs:
- layer_out: bfloat16 [2, 2048, 1024], P(None, 'dp', 'rep')
- gate_grad: bfloat16 [2, 2048, 5632], P(None, 'dp', 'rep')
- up_grad: bfloat16 [2, 2048, 5632], P(None, 'dp', 'rep')
- master_new: float32 [1024, 5632], P('dp', 'rep')
- moment_one_new: float32 [1024, 5632], P('dp', 'rep')
- moment_two_new: float32 [1024, 5632], P('dp', 'rep')
The draws below stay inside these ranges and needn't reach their ends.
All inputs are finite; a program needn't handle non-finite values.
Results may differ from the reference program's by a relative error of at most 0.0048.
The reference program's roundings to bfloat16 on the way (of `weight_bf` and `hidden`) count: a program that leaves them out, or rounds other values in their place, can miss the bound.
Values may be sent and summed in bfloat16 or wider, within the bound.
A program may use at most 128 MiB of HBM per device.

```python
import math
import jax
import jax.numpy as jnp
from jax import lax

D = 1024
FF = 5632
MB = 2
TOKENS = 2048


def strengthened(values, stream_key, source, target, shards_of, factor):
    def block_of(axis_at):
        return (jnp.arange(values.shape[axis_at]) // (values.shape[axis_at] // shards_of)).reshape((-1,) + (1,) * (values.ndim - 1 - axis_at))

    one_side = jax.random.permutation(stream_key, shards_of)[block_of(target)]
    far = (block_of(target) + shards_of // 2) % shards_of
    return jnp.where((block_of(source) == one_side) | (block_of(source) == far), factor * values, values)


def shard_levels(rng, shape, pieces, smallest, top_value):
    level, own = 1.0, jax.random.fold_in(rng, 6)
    for axis_at, blocks in pieces:
        draws = jnp.exp(jax.random.uniform(jax.random.fold_in(own, axis_at), (blocks,), jnp.float32, smallest / len(pieces), top_value / len(pieces)))
        level = level * jnp.repeat(draws, shape[axis_at] // blocks).reshape([-1 if axis == axis_at else 1 for axis in range(len(shape))])
    return level


def centred(rng, extent, width, most, pieces=(), held_as=jnp.bfloat16):
    array = jax.random.normal(rng, extent, jnp.float32) * width
    if len(pieces) > 0:
        array = shard_levels(rng, extent, pieces, -0.22, 0.18) * array
    return jnp.clip(array, min=-most, max=most).astype(held_as)


def heavy_noise(key, shape, scale, reach, pieces, heavy, dtype=jnp.bfloat16):
    drawn = scale * jax.random.normal(key, shape, jnp.float32)
    if pieces:
        drawn = drawn * shard_levels(key, shape, pieces, -0.22, 0.18)
    return jnp.clip(strengthened(drawn, jax.random.fold_in(key, 3), *heavy), -reach, reach).astype(dtype)


def setup_inputs(seed: int = 0) -> dict:
    splits = jax.random.split(jax.random.key(seed), 7)
    gate_pre = centred(splits[0], (MB, TOKENS, FF), 1.5, 8.0, ((1, 16), (2, 2)))
    up_pre = centred(splits[1], (MB, TOKENS, FF), 1.0, 6.0, ((1, 16), (2, 2)))
    out_grad = heavy_noise(splits[2], (MB, TOKENS, D), 1.0, 6.0, ((1, 16),), (1, 2, 16, 2.0))
    master = centred(splits[3], (D, FF), FF ** -0.5, 0.078125, ((0, 16), (1, 2)), jnp.float32)
    moment_one = centred(splits[4], (D, FF), 0.003, 0.02, ((0, 16), (1, 2)), jnp.float32)
    moment_two = jnp.clip(jnp.exp(math.log(9.999999747378752e-06) - 2.3025851 * jax.random.uniform(splits[5], (D, FF), jnp.float32) ** shard_levels(splits[5], (D, FF), ((0, 16), (1, 2)), -0.2, 0.2)), 9.999999974752427e-07, 9.999999747378752e-06)
    return {"gate_pre": gate_pre, "up_pre": up_pre, "out_grad": out_grad, "master": master, "moment_one": moment_one, "moment_two": moment_two}


first_power = 2.6561398887587544e-05
second_power = 0.005920529220333997

def reference(gate_pre, up_pre, out_grad, master, moment_one, moment_two):
    weight_bf = master.astype(jnp.bfloat16)
    outs_list = []
    gate_list = []
    up_list = []
    grad_sum = jnp.zeros(master.shape, jnp.float32)
    for index in range(MB):
        gate = gate_pre[index].astype(jnp.float32)
        up_val = up_pre[index].astype(jnp.float32)
        sig = jax.nn.sigmoid(gate)
        hidden = (gate * sig * up_val).astype(jnp.bfloat16)
        result = lax.dot_general(hidden, weight_bf, (((1,), (1,)), ((), ())), preferred_element_type=jnp.float32)
        outs_list.append(result.astype(jnp.bfloat16))
        hid_grad = jnp.dot(out_grad[index], weight_bf, preferred_element_type=jnp.float32)
        gate_list.append((hid_grad * up_val * sig * (1.0 + gate * (1.0 - sig))).astype(jnp.bfloat16))
        up_list.append((hid_grad * gate * sig).astype(jnp.bfloat16))
        grad_sum = grad_sum + lax.dot_general(out_grad[index], hidden, (((0,), (0,)), ((), ())), preferred_element_type=jnp.float32)
    main_grad = grad_sum / jnp.float32(MB * TOKENS)
    first = 0.9 * moment_one + 0.1 * main_grad
    second = 0.95 * moment_two + 0.05 * main_grad * main_grad
    update = first / (1.0 - first_power) / (jnp.sqrt(second / (1.0 - second_power)) + 1e-08)
    master_new = master - 0.003 * (update + 0.1 * master)
    return (jnp.stack(outs_list), jnp.stack(gate_list), jnp.stack(up_list), master_new, first, second)
```

```python
import functools

import jax
import jax.numpy as jnp
from jax import lax
from jax.experimental import pallas as pl
from jax.experimental.pallas import tpu as pltpu
from jax.sharding import PartitionSpec as P

first_power = 2.6561398887587544e-05
second_power = 0.005920529220333997

MESH = pl.DeviceIdType.MESH
CORES = 2
MID = 2


def adam(main_grad, master, moment_one, moment_two):
    first = 0.9 * moment_one + 0.1 * main_grad
    second = 0.95 * moment_two + 0.05 * main_grad * main_grad
    update = first / (1.0 - first_power) / (jnp.sqrt(second / (1.0 - second_power)) + 1e-08)
    return master - 0.003 * (update + 0.1 * master), first, second


def fused(
    outer, total,
    gate_ref, up_ref, cot_ref, cot_rows_ref, shard_ref, master_ref, one_ref, two_ref,
    out_ref, gate_grad_ref, up_grad_ref, master_new_ref, first_ref, second_ref,
    weights, hid, hid_peer, cot_peer, own_sum, mid_send, mid_recv, outer_send, outer_recv,
    part_send, part_recv,
    w_recv, w_mid_send, w_outer_send, w_core_send,
    core_send_sem, core_recv_sem,
    mid_send_sem, mid_recv_sem, outer_send_sem, outer_recv_sem, part_send_sem, part_recv_sem,
):
    me = lax.axis_index("dp")
    rep = lax.axis_index("rep")
    core = lax.rem(me, CORES)
    mid = lax.rem(me // CORES, MID)
    out = me // (CORES * MID)
    n = outer * MID * CORES
    rows, ff = shard_ref.shape
    tokens = gate_ref.shape[0]
    width = 256 if ff % 256 == 0 else 128
    chunks = ff // width

    def at(o, m, c):
        return (o * MID + m) * CORES + c

    core_peer = {"dp": at(out, mid, 1 - core)}
    mid_peer = {"dp": at(out, 1 - mid, core)}
    rep_peer = {"rep": 1 - rep}

    def outer_at(k):
        return lax.rem(out + k, outer)

    def outer_peer(k):
        return {"dp": at(outer_at(k), mid, core)}

    def remote(src, dst, send, recv, device):
        return pltpu.make_async_remote_copy(
            src_ref=src, dst_ref=dst, send_sem=send, recv_sem=recv,
            device_id=device, device_id_type=MESH,
        )

    barrier = pltpu.get_barrier_semaphore()
    peers = [core_peer, mid_peer, rep_peer] + [outer_peer(k) for k in range(1, outer)]
    for peer in peers:
        pl.semaphore_signal(barrier, inc=1, device_id=peer, device_id_type=MESH)
    pl.semaphore_wait(barrier, len(peers))

    order = sorted(range(1, outer), key=lambda k: min(k, outer - k))
    started = []

    def go(copy):
        copy.start()
        started.append(copy)
        return copy

    for k in order:
        go(remote(shard_ref, weights.at[me], w_outer_send.at[k], w_recv.at[me], outer_peer(k)))
    go(remote(shard_ref, weights.at[me], w_mid_send.at[0], w_recv.at[me], mid_peer))
    go(remote(shard_ref, weights.at[me], w_core_send.at[0], w_recv.at[me], core_peer))
    cot_copy = go(remote(cot_rows_ref.at[1 - core], cot_peer, core_send_sem.at[0], core_recv_sem.at[0], core_peer))
    weights[me] = shard_ref[...]

    def columns(j):
        return pl.ds(pl.multiple_of(j * width, width), width)

    def hidden_step(j, carry):
        cols = columns(j)
        gate = gate_ref[:, cols].astype(jnp.float32)
        sig = jax.nn.sigmoid(gate)
        hid[:, cols] = (gate * sig * up_ref[:, cols].astype(jnp.float32)).astype(jnp.bfloat16)
        return carry

    lax.fori_loop(0, chunks, hidden_step, 0)
    hid_copy = go(remote(hid, hid_peer, core_send_sem.at[1], core_recv_sem.at[1], core_peer))
    cot_copy.wait_recv()
    hid_copy.wait_recv()

    def grad_of(which, cols):
        own = cot_rows_ref[core, which].reshape(outer * rows, tokens)
        other = cot_peer[which].reshape(outer * rows, tokens)
        value = jnp.dot(own, hid[:, cols], preferred_element_type=jnp.float32)
        value += jnp.dot(other, hid_peer[:, cols], preferred_element_type=jnp.float32)
        return value.reshape(outer, rows, width)

    def send_step(j, carry):
        cols = columns(j)
        mid_send[:, :, cols] = grad_of(1 - mid, cols).astype(jnp.bfloat16)
        return carry

    lax.fori_loop(0, chunks, send_step, 0)
    shift = list(reversed(order)) + [0]
    for k in shift:
        slot = outer_at(k)
        go(remote(mid_send.at[slot], mid_recv.at[slot], mid_send_sem.at[k], mid_recv_sem.at[slot], mid_peer))

    def own_step(j, carry):
        cols = columns(j)
        own_sum[:, :, cols] = grad_of(mid, cols)
        return carry

    lax.fori_loop(0, chunks, own_step, 0)

    def arrival(slot):
        return remote(weights.at[slot], weights.at[slot], w_core_send.at[0], w_recv.at[slot], core_peer)

    def forward_outer(k):
        slot = at(lax.rem(out + outer - k, outer), mid, core)
        arrival(slot).wait_recv()
        go(remote(weights.at[slot], weights.at[slot], w_mid_send.at[k], w_recv.at[slot], mid_peer))
        go(remote(weights.at[slot], weights.at[slot], w_core_send.at[k], w_recv.at[slot], core_peer))

    def forward_mid(k):
        slot = at(lax.rem(out + outer - k, outer), 1 - mid, core)
        arrival(slot).wait_recv()
        go(remote(weights.at[slot], weights.at[slot], w_core_send.at[outer + k], w_recv.at[slot], core_peer))

    def mid_wait(slot):
        remote(mid_recv.at[slot], mid_recv.at[slot], mid_send_sem.at[0], mid_recv_sem.at[slot], mid_peer).wait_recv()

    def pass_on(k):
        slot = outer_at(k)
        mid_wait(slot)

        def step(j, carry):
            cols = columns(j)
            outer_send[slot, :, cols] = (
                own_sum[slot, :, cols] + mid_recv[slot, :, cols].astype(jnp.float32)
            ).astype(jnp.bfloat16)
            return carry

        lax.fori_loop(0, chunks, step, 0)
        go(remote(outer_send.at[slot], outer_recv.at[out], outer_send_sem.at[k], outer_recv_sem.at[out], outer_peer(k)))

    for k, back in zip(order, list(reversed(order))):
        forward_outer(k)
        pass_on(back)
    for k in [0] + order:
        forward_mid(k)
    for k in range(outer):
        for m in range(MID):
            arrival(at(outer_at(k), m, 1 - core)).wait_recv()

    half = n // 2
    group = max(1, min(half, 256 // rows))

    def part_step(base, target):
        def step(g, carry):
            some = weights[pl.ds(base + g * group, group)].reshape(group * rows, ff)
            target[g] = lax.dot_general(
                hid[...], some, (((1,), (1,)), ((), ())), preferred_element_type=jnp.float32
            )
            return carry

        lax.fori_loop(0, half // group, step, 0)

    part_step((1 - rep) * half, part_send)
    part_copy = go(remote(part_send, part_recv, part_send_sem, part_recv_sem, rep_peer))

    def input_step(j, carry):
        cols = columns(j)
        grad = jnp.dot(
            cot_ref[...], weights[:, :, cols].reshape(n * rows, width),
            preferred_element_type=jnp.float32,
        )
        gate = gate_ref[:, cols].astype(jnp.float32)
        up_val = up_ref[:, cols].astype(jnp.float32)
        sig = jax.nn.sigmoid(gate)
        gate_grad_ref[:, cols] = (grad * up_val * sig * (1.0 + gate * (1.0 - sig))).astype(jnp.bfloat16)
        up_grad_ref[:, cols] = (grad * gate * sig).astype(jnp.bfloat16)
        return carry

    lax.fori_loop(0, chunks, input_step, 0)

    part_copy.wait_recv()
    base = rep * half
    for g in range(half // group):
        some = weights[pl.ds(base + g * group, group)].reshape(group * rows, ff)
        own = lax.dot_general(
            hid[...], some, (((1,), (1,)), ((), ())), preferred_element_type=jnp.float32
        )
        out_ref[:, g * group * rows : (g + 1) * group * rows] = (own + part_recv[g]).astype(jnp.bfloat16)

    mid_wait(out)
    sources = [lax.rem(out + outer - k, outer) for k in range(1, outer)]
    for source in sources:
        remote(outer_recv.at[source], outer_recv.at[source], outer_send_sem.at[0], outer_recv_sem.at[source], mid_peer).wait_recv()

    def update_step(j, carry):
        cols = columns(j)
        grad = own_sum[out, :, cols] + mid_recv[out, :, cols].astype(jnp.float32)
        for source in sources:
            grad += outer_recv[source, :, cols].astype(jnp.float32)
        master_new, first, second = adam(
            grad / jnp.float32(total), master_ref[:, cols], one_ref[:, cols], two_ref[:, cols]
        )
        master_new_ref[:, cols] = master_new
        first_ref[:, cols] = first
        second_ref[:, cols] = second
        return carry

    lax.fori_loop(0, chunks, update_step, 0)
    for copy in started:
        copy.wait_send()


def in_one_kernel(size, gate_pre, up_pre, out_grad, master, moment_one, moment_two):
    micro, count, ff = gate_pre.shape
    tokens, depth, rows = micro * count, out_grad.shape[2], master.shape[0]
    outer = size // (MID * CORES)
    half = size // 2
    group = max(1, min(half, 256 // rows))
    cot = out_grad.reshape(tokens, depth)
    cot_rows = jnp.transpose(cot.reshape(tokens, outer, MID, CORES, rows), (3, 2, 1, 4, 0))
    vmem = pl.BlockSpec(memory_space=pltpu.VMEM)
    bf, f32 = jnp.bfloat16, jnp.float32
    dma = pltpu.SemaphoreType.DMA
    results = pl.pallas_call(
        functools.partial(fused, outer, tokens * size),
        out_shape=(
            jax.ShapeDtypeStruct((tokens, depth // 2), bf),
            jax.ShapeDtypeStruct((tokens, ff), bf),
            jax.ShapeDtypeStruct((tokens, ff), bf),
            jax.ShapeDtypeStruct((rows, ff), f32),
            jax.ShapeDtypeStruct((rows, ff), f32),
            jax.ShapeDtypeStruct((rows, ff), f32),
        ),
        in_specs=[vmem] * 8,
        out_specs=(vmem,) * 6,
        scratch_shapes=[
            pltpu.VMEM((size, rows, ff), bf),
            pltpu.VMEM((tokens, ff), bf),
            pltpu.VMEM((tokens, ff), bf),
            pltpu.VMEM((MID, outer, rows, tokens), bf),
            pltpu.VMEM((outer, rows, ff), f32),
            pltpu.VMEM((outer, rows, ff), bf),
            pltpu.VMEM((outer, rows, ff), bf),
            pltpu.VMEM((outer, rows, ff), bf),
            pltpu.VMEM((outer, rows, ff), bf),
            pltpu.VMEM((half // group, tokens, group * rows), f32),
            pltpu.VMEM((half // group, tokens, group * rows), f32),
            dma((size,)), dma((outer,)), dma((outer,)), dma((2 * outer,)),
            dma((2,)), dma((2,)),
            dma((outer,)), dma((outer,)), dma((outer,)), dma((outer,)), dma, dma,
        ],
        compiler_params=pltpu.CompilerParams(
            collective_id=0, has_side_effects=True, vmem_limit_bytes=60 * 1024 * 1024
        ),
    )(
        gate_pre.reshape(tokens, ff), up_pre.reshape(tokens, ff), cot, cot_rows,
        master.astype(bf), master, moment_one, moment_two,
    )
    split = [value.reshape(micro, count, value.shape[1]) for value in results[:3]]
    return (*split, *results[3:])


def with_collectives(gate_pre, up_pre, out_grad, master, moment_one, moment_two):
    weights = lax.all_gather(master.astype(jnp.bfloat16), "dp", axis=0, tiled=True)
    micro = gate_pre.shape[0]
    total = micro * gate_pre.shape[1] * lax.axis_size("dp")
    outs_list = []
    gate_list = []
    up_list = []
    grad_sum = None
    for index in range(micro):
        gate = gate_pre[index].astype(jnp.float32)
        up_val = up_pre[index].astype(jnp.float32)
        sig = jax.nn.sigmoid(gate)
        hidden = (gate * sig * up_val).astype(jnp.bfloat16)
        partial_out = lax.dot_general(
            hidden, weights, (((1,), (1,)), ((), ())), preferred_element_type=jnp.float32
        )
        outs_list.append(
            lax.psum_scatter(partial_out, "rep", scatter_dimension=1, tiled=True).astype(
                jnp.bfloat16
            )
        )
        hid_grad = jnp.dot(out_grad[index], weights, preferred_element_type=jnp.float32)
        gate_list.append(
            (hid_grad * up_val * sig * (1.0 + gate * (1.0 - sig))).astype(jnp.bfloat16)
        )
        up_list.append((hid_grad * gate * sig).astype(jnp.bfloat16))
        term = lax.dot_general(
            out_grad[index], hidden, (((0,), (0,)), ((), ())), preferred_element_type=jnp.float32
        )
        shard = lax.psum_scatter(term, "dp", scatter_dimension=0, tiled=True)
        grad_sum = shard if grad_sum is None else grad_sum + shard
    updated = adam(grad_sum / jnp.float32(total), master, moment_one, moment_two)
    return jnp.stack(outs_list), jnp.stack(gate_list), jnp.stack(up_list), *updated


def solution(mesh):
    size = mesh.shape["dp"]

    def on_device(gate_pre, up_pre, out_grad, master, moment_one, moment_two):
        tall = master.shape[0] % 16 == 0 and size % (MID * CORES) == 0
        step = functools.partial(in_one_kernel, size) if tall else with_collectives
        return step(gate_pre, up_pre, out_grad, master, moment_one, moment_two)

    split = P(None, "dp", "rep")
    owned = P("dp", "rep")
    return jax.shard_map(
        on_device,
        mesh=mesh,
        in_specs=(split, split, P(None, "dp", None), owned, owned, owned),
        out_specs=(split, split, split, owned, owned, owned),
        check_vma=False,
    )
```

```python
import functools

import jax
import jax.numpy as jnp
from jax import lax
from jax.experimental import pallas as pl
from jax.experimental.pallas import tpu as pltpu
from jax.sharding import PartitionSpec as P

first_power = 2.6561398887587544e-05
second_power = 0.005920529220333997

MESH = pl.DeviceIdType.MESH
CORES = 2
MID = 2


def adam(main_grad, master, moment_one, moment_two):
    first = 0.9 * moment_one + 0.1 * main_grad
    second = 0.95 * moment_two + 0.05 * main_grad * main_grad
    update = first / (1.0 - first_power) / (jnp.sqrt(second / (1.0 - second_power)) + 1e-08)
    return master - 0.003 * (update + 0.1 * master), first, second


def fused(
    outer, total,
    gate_hbm, up_hbm, cot_ref, master_ref, one_hbm, two_hbm,
    out_ref, gate_grad_ref, up_grad_ref, master_new_ref, first_ref, second_ref,
    weights, hid, hid_peer, cot_peer, own_sum, mid_send, mid_recv, outer_send, outer_recv,
    part_send, part_recv, cot_rows_ref, gate_ref, up_ref, one_ref, two_ref, local_sem,
    w_recv, w_mid_send, w_outer_send, w_core_send,
    core_send_sem, core_recv_sem,
    mid_send_sem, mid_recv_sem, outer_send_sem, outer_recv_sem, part_send_sem, part_recv_sem,
):
    me = lax.axis_index("dp")
    rep = lax.axis_index("rep")
    core = lax.rem(me, CORES)
    mid = lax.rem(me // CORES, MID)
    out = me // (CORES * MID)
    n = outer * MID * CORES
    rows, ff = master_ref.shape
    tokens = gate_ref.shape[0]
    loads = [
        pltpu.make_async_copy(src, dst, local_sem.at[index])
        for index, (src, dst) in enumerate(
            ((gate_hbm, gate_ref), (up_hbm, up_ref), (one_hbm, one_ref), (two_hbm, two_ref))
        )
    ]
    for load in loads:
        load.start()
    width = 256 if ff % 256 == 0 else 128
    chunks = ff // width

    def at(o, m, c):
        return (o * MID + m) * CORES + c

    core_peer = {"dp": at(out, mid, 1 - core)}
    mid_peer = {"dp": at(out, 1 - mid, core)}
    rep_peer = {"rep": 1 - rep}

    def outer_at(k):
        return lax.rem(out + k, outer)

    def outer_peer(k):
        return {"dp": at(outer_at(k), mid, core)}

    def remote(src, dst, send, recv, device):
        return pltpu.make_async_remote_copy(
            src_ref=src, dst_ref=dst, send_sem=send, recv_sem=recv,
            device_id=device, device_id_type=MESH,
        )

    weights[me] = master_ref[...].astype(jnp.bfloat16)
    barrier = pltpu.get_barrier_semaphore()
    peers = [core_peer, mid_peer, rep_peer] + [outer_peer(k) for k in range(1, outer)]
    for peer in peers:
        pl.semaphore_signal(barrier, inc=1, device_id=peer, device_id_type=MESH)
    pl.semaphore_wait(barrier, len(peers))

    order = sorted(range(1, outer), key=lambda k: min(k, outer - k))
    started = []

    def go(copy):
        copy.start()
        started.append(copy)
        return copy

    for k in order:
        go(remote(weights.at[me], weights.at[me], w_outer_send.at[k], w_recv.at[me], outer_peer(k)))
    go(remote(weights.at[me], weights.at[me], w_mid_send.at[0], w_recv.at[me], mid_peer))
    go(remote(weights.at[me], weights.at[me], w_core_send.at[0], w_recv.at[me], core_peer))
    turned = jnp.transpose(cot_ref[...].astype(jnp.float32)).astype(jnp.bfloat16).reshape(n, rows, tokens)
    for o in range(outer):
        for m in range(MID):
            for c in range(CORES):
                cot_rows_ref[c, m, o] = turned[at(o, m, c)]
    loads[0].wait()
    loads[1].wait()

    def columns(j):
        return pl.ds(pl.multiple_of(j * width, width), width)

    def hidden_step(j, carry):
        cols = columns(j)
        gate = gate_ref[:, cols].astype(jnp.float32)
        sig = jax.nn.sigmoid(gate)
        hid[:, cols] = (gate * sig * up_ref[:, cols].astype(jnp.float32)).astype(jnp.bfloat16)
        return carry

    lax.fori_loop(0, chunks, hidden_step, 0)
    cot_copy = go(remote(cot_rows_ref.at[1 - core], cot_peer, core_send_sem.at[0], core_recv_sem.at[0], core_peer))
    hid_copy = go(remote(hid, hid_peer, core_send_sem.at[1], core_recv_sem.at[1], core_peer))
    cot_copy.wait_recv()
    hid_copy.wait_recv()

    def grad_of(which, cols):
        own = cot_rows_ref[core, which].reshape(outer * rows, tokens)
        other = cot_peer[which].reshape(outer * rows, tokens)
        value = jnp.dot(own, hid[:, cols], preferred_element_type=jnp.float32)
        value += jnp.dot(other, hid_peer[:, cols], preferred_element_type=jnp.float32)
        return value.reshape(outer, rows, width)

    def send_step(j, carry):
        cols = columns(j)
        mid_send[:, :, cols] = grad_of(1 - mid, cols).astype(jnp.bfloat16)
        return carry

    lax.fori_loop(0, chunks, send_step, 0)

    def reduce_mid(k):
        slot = outer_at(k)
        go(remote(mid_send.at[slot], mid_recv.at[slot], mid_send_sem.at[k], mid_recv_sem.at[slot], mid_peer))

    def arrival(slot):
        return remote(weights.at[slot], weights.at[slot], w_core_send.at[0], w_recv.at[slot], core_peer)

    def forward_outer(k):
        slot = at(lax.rem(out + outer - k, outer), mid, core)
        arrival(slot).wait_recv()
        go(remote(weights.at[slot], weights.at[slot], w_mid_send.at[k], w_recv.at[slot], mid_peer))
        go(remote(weights.at[slot], weights.at[slot], w_core_send.at[k], w_recv.at[slot], core_peer))

    def forward_mid(k):
        slot = at(lax.rem(out + outer - k, outer), 1 - mid, core)
        arrival(slot).wait_recv()
        go(remote(weights.at[slot], weights.at[slot], w_core_send.at[outer + k], w_recv.at[slot], core_peer))

    def mid_wait(slot):
        remote(mid_recv.at[slot], mid_recv.at[slot], mid_send_sem.at[0], mid_recv_sem.at[slot], mid_peer).wait_recv()

    def pass_on(k):
        slot = outer_at(k)
        mid_wait(slot)

        def step(j, carry):
            cols = columns(j)
            outer_send[slot, :, cols] = (
                own_sum[slot, :, cols] + mid_recv[slot, :, cols].astype(jnp.float32)
            ).astype(jnp.bfloat16)
            return carry

        lax.fori_loop(0, chunks, step, 0)
        go(remote(outer_send.at[slot], outer_recv.at[out], outer_send_sem.at[k], outer_recv_sem.at[out], outer_peer(k)))

    back = list(reversed(order))
    forward_outer(order[0])
    reduce_mid(back[0])
    def own_step(j, carry):
        cols = columns(j)
        own_sum[:, :, cols] = grad_of(mid, cols)
        return carry

    lax.fori_loop(0, chunks, own_step, 0)

    forward_mid(0)
    for index in range(1, outer - 1):
        forward_outer(order[index])
        reduce_mid(back[index])
        if index < outer - 2:
            pass_on(back[index - 1])
    reduce_mid(0)
    for k in order[:-1]:
        forward_mid(k)
    if outer > 2:
        pass_on(back[-2])
    forward_mid(order[-1])
    for k in range(outer):
        for m in range(MID):
            arrival(at(outer_at(k), m, 1 - core)).wait_recv()

    half = n // 2
    group = max(1, min(half, 256 // rows))

    def part_step(base, target):
        def step(g, carry):
            some = weights[pl.ds(base + g * group, group)].reshape(group * rows, ff)
            target[g] = lax.dot_general(
                hid[...], some, (((1,), (1,)), ((), ())), preferred_element_type=jnp.float32
            )
            return carry

        lax.fori_loop(0, half // group, step, 0)

    part_step((1 - rep) * half, part_send)
    part_copy = go(remote(part_send, part_recv, part_send_sem, part_recv_sem, rep_peer))

    def input_step(j, carry):
        cols = columns(j)
        grad = jnp.dot(
            cot_ref[...], weights[:, :, cols].reshape(n * rows, width),
            preferred_element_type=jnp.float32,
        )
        gate = gate_ref[:, cols].astype(jnp.float32)
        up_val = up_ref[:, cols].astype(jnp.float32)
        sig = jax.nn.sigmoid(gate)
        gate_grad_ref[:, cols] = (grad * up_val * sig * (1.0 + gate * (1.0 - sig))).astype(jnp.bfloat16)
        up_grad_ref[:, cols] = (grad * gate * sig).astype(jnp.bfloat16)
        return carry

    lax.fori_loop(0, chunks // 2, input_step, 0)
    pass_on(back[-1])
    lax.fori_loop(chunks // 2, chunks, input_step, 0)

    part_copy.wait_recv()
    base = rep * half
    for g in range(half // group):
        some = weights[pl.ds(base + g * group, group)].reshape(group * rows, ff)
        own = lax.dot_general(
            hid[...], some, (((1,), (1,)), ((), ())), preferred_element_type=jnp.float32
        )
        out_ref[:, g * group * rows : (g + 1) * group * rows] = (own + part_recv[g]).astype(jnp.bfloat16)

    mid_wait(out)
    sources = [lax.rem(out + outer - k, outer) for k in range(1, outer)]
    for source in sources:
        remote(outer_recv.at[source], outer_recv.at[source], outer_send_sem.at[0], outer_recv_sem.at[source], mid_peer).wait_recv()

    loads[2].wait()
    loads[3].wait()

    def update_step(j, carry):
        cols = columns(j)
        grad = own_sum[out, :, cols] + mid_recv[out, :, cols].astype(jnp.float32)
        for source in sources:
            grad += outer_recv[source, :, cols].astype(jnp.float32)
        master_new, first, second = adam(
            grad / jnp.float32(total), master_ref[:, cols], one_ref[:, cols], two_ref[:, cols]
        )
        master_new_ref[:, cols] = master_new
        first_ref[:, cols] = first
        second_ref[:, cols] = second
        return carry

    lax.fori_loop(0, chunks, update_step, 0)
    for copy in started:
        copy.wait_send()


def in_one_kernel(size, gate_pre, up_pre, out_grad, master, moment_one, moment_two):
    micro, count, ff = gate_pre.shape
    tokens, depth, rows = micro * count, out_grad.shape[2], master.shape[0]
    outer = size // (MID * CORES)
    half = size // 2
    group = max(1, min(half, 256 // rows))
    cot = out_grad.reshape(tokens, depth)
    vmem = pl.BlockSpec(memory_space=pltpu.VMEM)
    hbm = pl.BlockSpec(memory_space=pl.ANY)
    bf, f32 = jnp.bfloat16, jnp.float32
    dma = pltpu.SemaphoreType.DMA
    results = pl.pallas_call(
        functools.partial(fused, outer, tokens * size),
        out_shape=(
            jax.ShapeDtypeStruct((tokens, depth // 2), bf),
            jax.ShapeDtypeStruct((tokens, ff), bf),
            jax.ShapeDtypeStruct((tokens, ff), bf),
            jax.ShapeDtypeStruct((rows, ff), f32),
            jax.ShapeDtypeStruct((rows, ff), f32),
            jax.ShapeDtypeStruct((rows, ff), f32),
        ),
        in_specs=[hbm, hbm, vmem, vmem, hbm, hbm],
        out_specs=(vmem,) * 6,
        scratch_shapes=[
            pltpu.VMEM((size, rows, ff), bf),
            pltpu.VMEM((tokens, ff), bf),
            pltpu.VMEM((tokens, ff), bf),
            pltpu.VMEM((MID, outer, rows, tokens), bf),
            pltpu.VMEM((outer, rows, ff), f32),
            pltpu.VMEM((outer, rows, ff), bf),
            pltpu.VMEM((outer, rows, ff), bf),
            pltpu.VMEM((outer, rows, ff), bf),
            pltpu.VMEM((outer, rows, ff), bf),
            pltpu.VMEM((half // group, tokens, group * rows), f32),
            pltpu.VMEM((half // group, tokens, group * rows), f32),
            pltpu.VMEM((CORES, MID, outer, rows, tokens), bf),
            pltpu.VMEM((tokens, ff), bf),
            pltpu.VMEM((tokens, ff), bf),
            pltpu.VMEM((rows, ff), f32),
            pltpu.VMEM((rows, ff), f32),
            dma((4,)),
            dma((size,)), dma((outer,)), dma((outer,)), dma((2 * outer,)),
            dma((2,)), dma((2,)),
            dma((outer,)), dma((outer,)), dma((outer,)), dma((outer,)), dma, dma,
        ],
        compiler_params=pltpu.CompilerParams(
            collective_id=0, has_side_effects=True, vmem_limit_bytes=60 * 1024 * 1024
        ),
    )(
        gate_pre.reshape(tokens, ff), up_pre.reshape(tokens, ff), cot, master, moment_one, moment_two,
    )
    split = [value.reshape(micro, count, value.shape[1]) for value in results[:3]]
    return (*split, *results[3:])


def with_collectives(gate_pre, up_pre, out_grad, master, moment_one, moment_two):
    weights = lax.all_gather(master.astype(jnp.bfloat16), "dp", axis=0, tiled=True)
    micro = gate_pre.shape[0]
    total = micro * gate_pre.shape[1] * lax.axis_size("dp")
    outs_list = []
    gate_list = []
    up_list = []
    grad_sum = None
    for index in range(micro):
        gate = gate_pre[index].astype(jnp.float32)
        up_val = up_pre[index].astype(jnp.float32)
        sig = jax.nn.sigmoid(gate)
        hidden = (gate * sig * up_val).astype(jnp.bfloat16)
        partial_out = lax.dot_general(
            hidden, weights, (((1,), (1,)), ((), ())), preferred_element_type=jnp.float32
        )
        outs_list.append(
            lax.psum_scatter(partial_out, "rep", scatter_dimension=1, tiled=True).astype(
                jnp.bfloat16
            )
        )
        hid_grad = jnp.dot(out_grad[index], weights, preferred_element_type=jnp.float32)
        gate_list.append(
            (hid_grad * up_val * sig * (1.0 + gate * (1.0 - sig))).astype(jnp.bfloat16)
        )
        up_list.append((hid_grad * gate * sig).astype(jnp.bfloat16))
        term = lax.dot_general(
            out_grad[index], hidden, (((0,), (0,)), ((), ())), preferred_element_type=jnp.float32
        )
        shard = lax.psum_scatter(term, "dp", scatter_dimension=0, tiled=True)
        grad_sum = shard if grad_sum is None else grad_sum + shard
    updated = adam(grad_sum / jnp.float32(total), master, moment_one, moment_two)
    return jnp.stack(outs_list), jnp.stack(gate_list), jnp.stack(up_list), *updated


def solution(mesh):
    size = mesh.shape["dp"]

    def on_device(gate_pre, up_pre, out_grad, master, moment_one, moment_two):
        tall = master.shape[0] % 16 == 0 and size % (MID * CORES) == 0 and size > MID * CORES
        step = functools.partial(in_one_kernel, size) if tall else with_collectives
        return step(gate_pre, up_pre, out_grad, master, moment_one, moment_two)

    split = P(None, "dp", "rep")
    owned = P("dp", "rep")
    return jax.shard_map(
        on_device,
        mesh=mesh,
        in_specs=(split, split, P(None, "dp", None), owned, owned, owned),
        out_specs=(split, split, split, owned, owned, owned),
        check_vma=False,
    )
```
